32 devices in a mesh: gx: 4 (over x, core), gy: 8 (over z, y).
Axes of the slice: x: 2, y: 2, z: 4, core: 2. Of those that a mesh axis runs over, the one named last changes fastest.
Arguments:
- slot_tiles: int32 [32, 32], P(('gx', 'gy')), may hold values from -1 to 63, as said below
- owner_map: int32 [32], replicated, may hold values from 0 to 31, each once
- slot_depth: int32 [32, 32, 16, 128], P(('gx', 'gy')), may hold values from 0 to 1073741823
- slot_color: bfloat16 [32, 32, 16, 3, 128], P(('gx', 'gy')), may hold values from 0 to 1
Outputs:
- region_depth: int32 [32, 2, 16, 128], P(('gx', 'gy'))
- region_color: bfloat16 [32, 2, 16, 3, 128], P(('gx', 'gy'))
- thumbnail: float32 [32, 3, 64], replicated
The draws below stay inside these ranges and needn't reach their ends.
Inputs may be any that keep to these rules, and one draw needn't show every extreme that they name: `slot_tiles`: each rank's used slots name the tiles of one rectangle of at least 4 tile rows of the 8 x 8 tile grid, each once, in row-major order, followed by -1 in the unused slots; all ranks' rectangles contain a common region. `owner_map`: each rank owns exactly one region.
All inputs are finite; a program needn't handle non-finite values.
Results may differ from the reference program's by a relative error of at most 0.001.
Values may be sent and summed in bfloat16 or wider, within the bound.
No kernel may reach another device: no remote copies, remote signals or barrier semaphores. Data moves between devices by JAX's collectives and lax.ppermute only.
A program may use at most 64 MiB of HBM per device.

```python
import jax
import jax.numpy as jnp
from jax import lax

TILE = 128
BAND = 16
TROWS = 8
TCOLS = 8
TILES = 64
SLOTS = 32
REGIONS = 32
THUMB = 64
DEVICES = 32


def box_tiles(key):
    keys = jax.random.split(jax.random.fold_in(key, 11), 9)
    focus_pair = jax.random.randint(keys[0], (), 0, TROWS // 2)
    focus_col = jax.random.randint(keys[1], (), 0, TCOLS)
    lowest = max(3, TROWS // 2)
    box_height = lowest + jax.random.randint(keys[2], (DEVICES,), 0, 1 << 20) % (TROWS - lowest + 1)
    widest = jnp.minimum(SLOTS // box_height, TCOLS)
    narrowing = jax.random.randint(keys[8], (DEVICES,), 0, 2)
    box_width = jnp.maximum(1, widest - narrowing)
    row_low = jnp.maximum(0, 2 * focus_pair + 2 - box_height)
    row_high = jnp.minimum(2 * focus_pair, TROWS - box_height)
    row_span = row_high - row_low + 1
    first_draw = jax.random.randint(keys[4], (DEVICES,), 0, 1 << 20) % row_span
    second_draw = jax.random.randint(keys[5], (DEVICES,), 0, 1 << 20) % row_span
    top_row = row_low + (first_draw + second_draw) // 2
    col_low = jnp.maximum(0, focus_col - box_width + 1)
    col_high = jnp.minimum(focus_col, TCOLS - box_width)
    col_span = col_high - col_low + 1
    third_draw = jax.random.randint(keys[6], (DEVICES,), 0, 1 << 20) % col_span
    fourth_draw = jax.random.randint(keys[7], (DEVICES,), 0, 1 << 20) % col_span
    left_col = col_low + (third_draw + fourth_draw) // 2
    slot_index = jnp.arange(SLOTS, dtype=jnp.int32)[None, :]
    inner_row = slot_index // box_width[:, None]
    inner_col = slot_index % box_width[:, None]
    is_live = slot_index < (box_height * box_width)[:, None]
    tile_ids = (top_row[:, None] + inner_row) * TCOLS + left_col[:, None] + inner_col
    return jnp.where(is_live, tile_ids, -1).astype(jnp.int32)


def draw_slot_tiles(key, part):
    return box_tiles(key)


def draw_slot_depth(key, part):
    tile_ids = box_tiles(key)
    keys = jax.random.split(jax.random.fold_in(key, 23), 3)
    surface = jax.random.randint(keys[0], (TILES, BAND, TILE), 0, 1073741823).astype(jnp.int32)
    safe_tile = jnp.where(tile_ids >= 0, tile_ids, 0).astype(jnp.int32)
    front = surface[safe_tile]
    coin = jax.random.randint(keys[1], (DEVICES, SLOTS, BAND, TILE), 0, 8)
    room = (1073741823 - front).astype(jnp.int32)
    raw_extra = jax.random.randint(keys[2], (DEVICES, SLOTS, BAND, TILE), 0, 1 << 30).astype(jnp.int32)
    extra = 1 + raw_extra % room
    return (front + jnp.where(coin == 0, 0, extra)).astype(jnp.int32)


def block_levels(own_key, extent, shards, least, top_value):
    factor_of, own = 1.0, jax.random.fold_in(own_key, 6)
    for position, parts in shards:
        steps = jnp.exp(jax.random.uniform(jax.random.fold_in(own, position), (parts,), jnp.float32, least / len(shards), top_value / len(shards)))
        factor_of = factor_of * jnp.repeat(steps, extent[position] // parts).reshape([-1 if axis == position else 1 for axis in range(len(extent))])
    return factor_of


def setup_inputs(seed: int = 0) -> dict:
    seeds = jax.random.split(jax.random.key(seed), 5)
    return {
        "slot_tiles": draw_slot_tiles(jax.random.fold_in(seeds[4], 71), 0),
        "owner_map": jax.random.permutation(seeds[1], REGIONS).astype(jnp.int32),
        "slot_depth": draw_slot_depth(jax.random.fold_in(seeds[4], 71), 0),
        "slot_color": jnp.clip(1.0 * jax.random.uniform(seeds[3], (DEVICES, SLOTS, BAND, 3, TILE), jnp.float32) ** block_levels(seeds[3], (DEVICES, SLOTS, BAND, 3, TILE), ((0, 32),), -0.2, 0.2), 0.0, 1.0).astype(jnp.bfloat16),
    }


far_depth = 1073741824


def reference(slot_tiles, owner_map, slot_depth, slot_color):
    tile_count = TROWS * TCOLS

    def place_rank(frame_state, rank_data):
        frame_depth, frame_color = frame_state
        rank_tiles, rank_depth, rank_color = rank_data
        gather_index = jnp.where(rank_tiles >= 0, rank_tiles, tile_count).astype(jnp.int32)
        current = frame_depth[gather_index]
        nearer = rank_depth < current
        new_depth = jnp.where(nearer, rank_depth, current)
        new_color = jnp.where(nearer[:, :, None, :], rank_color, frame_color[gather_index])
        return (frame_depth.at[gather_index].set(new_depth), frame_color.at[gather_index].set(new_color)), None

    start_depth = jnp.full((tile_count + 1, BAND, TILE), far_depth, jnp.int32)
    start_color = jnp.zeros((tile_count + 1, BAND, 3, TILE), jnp.bfloat16)
    final_state, unused = lax.scan(place_rank, (start_depth, start_color), (slot_tiles, slot_depth, slot_color))
    frame_depth = final_state[0][:tile_count]
    frame_color = final_state[1][:tile_count]
    by_region_depth = jnp.transpose(frame_depth.reshape(TROWS // 2, 2, TCOLS, BAND, TILE), (0, 2, 1, 3, 4)).reshape(REGIONS, 2, BAND, TILE)
    by_region_color = jnp.transpose(frame_color.reshape(TROWS // 2, 2, TCOLS, BAND, 3, TILE), (0, 2, 1, 3, 4, 5)).reshape(REGIONS, 2, BAND, 3, TILE)
    inverse = jnp.zeros((REGIONS,), jnp.int32).at[owner_map].set(jnp.arange(REGIONS, dtype=jnp.int32))
    region_depth = by_region_depth[inverse]
    region_color = by_region_color[inverse]
    block_means = by_region_color.astype(jnp.float32).reshape(REGIONS, 2, BAND // 8, 8, 3, TILE // 8, 8).mean(axis=(3, 6))
    thumbnail = jnp.transpose(block_means, (0, 3, 1, 2, 4)).reshape(REGIONS, 3, THUMB)
    return region_depth, region_color, thumbnail
```

```python
import jax
import jax.numpy as jnp
import numpy as np
from jax import lax
from jax.experimental import pallas as pl
from jax.experimental.pallas import tpu as pltpu
from jax.sharding import PartitionSpec as P

far_depth = 1073741824
depth_shift = 536870912
axes = ("gx", "gy")
smem = pl.BlockSpec(memory_space=pltpu.SMEM)
vmem = pl.BlockSpec(memory_space=pltpu.VMEM)


def paired_masks(low, high):
    masks = []
    bit = low
    if (high - low) % 2:
        masks.append(1 << bit)
        bit += 1
    while bit < high:
        masks.append(1 << bit)
        masks.append(3 << bit)
        bit += 2
    return masks


def exchange_plan(grid_rows, grid_cols):
    col_bits = grid_cols.bit_length() - 1
    row_bits = grid_rows.bit_length() - 1
    masks = [grid_cols]
    masks += paired_masks(0, col_bits)
    masks += paired_masks(col_bits + 1, col_bits + row_bits)
    return masks


def position_table(masks, ranks):
    table = np.zeros((ranks,), np.int32)
    steps = len(masks)
    for place in range(ranks):
        x = 0
        for step, mask in enumerate(masks):
            if place >> (steps - 1 - step) & 1:
                x ^= mask
        table[x] = place
    return table


def gather_table(masks, ranks):
    table = np.zeros((ranks,), np.int32)
    for place in range(ranks):
        x = 0
        for step, mask in enumerate(masks):
            if place >> step & 1:
                x ^= mask
        table[x] = place
    return table


def pack_kernel(grid_cols, rank_ref, tiles_ref, owner_ref, table_ref, depth_ref, color_ref, *refs):
    keep_d, keep_c, send_d, send_c, source_ref = refs
    slots = depth_ref.shape[0]
    half = keep_d.shape[0]

    def clear(p, carry):
        source_ref[p] = -1
        return carry

    lax.fori_loop(0, 2 * half, clear, 0, unroll=8)
    rank = rank_ref[0]

    def place(i, carry):
        tile = tiles_ref[0, i]

        @pl.when(tile >= 0)
        def _():
            row = lax.div(tile, grid_cols)
            col = lax.rem(tile, grid_cols)
            owner = owner_ref[(row >> 1) * grid_cols + col]
            source_ref[table_ref[owner ^ rank] * 2 + (row & 1)] = i

        return carry

    lax.fori_loop(0, slots, place, 0)

    def move(base, out_d, out_c):
        def body(p, carry):
            source = source_ref[base + p]
            used = source >= 0
            slot = jnp.maximum(source, 0)
            out_d[p] = jnp.where(used, depth_ref[slot], far_depth)
            color = color_ref[slot]
            out_c[p] = jnp.where(used, color, jnp.zeros_like(color))
            return carry

        lax.fori_loop(0, half, body, 0, unroll=4)

    move(half, send_d, send_c)
    move(0, keep_d, keep_c)


def pick(take, new_color, old_color):
    chosen = jnp.where(take[None], new_color.astype(jnp.float32), old_color.astype(jnp.float32))
    return chosen.astype(old_color.dtype)


def merge_kernel(bit, kind, rank_ref, own_d, own_c, got_d, got_c, *outs):
    later = (rank_ref[0] >> bit) & 1
    count = own_d.shape[0]
    half = count // 2 if len(outs) == 4 else count

    def merge(base, out_d, out_c):
        def body(p, carry):
            mine = own_d[base + p]
            other = got_d[base + p]
            if kind == "key":
                mine = (mine - depth_shift) * 2 + later
                other = (other - depth_shift) * 2 + (1 - later)
                take = other < mine
            elif kind == "order":
                take = other < mine + later
            else:
                take = (other >> 1) < (mine >> 1) + later
            out_d[p] = jnp.where(take, other, mine)
            out_c[p] = pick(take, got_c[base + p], own_c[base + p])
            return carry

        lax.fori_loop(0, half, body, 0, unroll=2)

    if len(outs) == 4:
        merge(half, outs[2], outs[3])
    merge(0, outs[0], outs[1])


def last_kernel(bit, rank_ref, own_d, own_c, got_d, got_c, out_d, out_c, thumb_ref):
    later = (rank_ref[0] >> bit) & 1
    lanes = own_d.shape[-1]
    rows = own_d.shape[-2]
    blocks = lanes // 8
    bands = rows // 8
    width = 2 * bands * blocks
    lane = lax.broadcasted_iota(jnp.int32, (lanes, width), 0) // 8
    place = lax.broadcasted_iota(jnp.int32, (lanes, width), 1)
    for region in range(2):
        total = jnp.zeros((3, width), jnp.float32)
        for h in range(2):
            mine = own_d[2 * region + h]
            other = got_d[2 * (1 - region) + h]
            take = (other >> 1) < (mine >> 1) + later
            color = jnp.where(
                take[None],
                got_c[2 * (1 - region) + h].astype(jnp.float32),
                own_c[2 * region + h].astype(jnp.float32),
            )
            if region == 0:
                out_d[h] = (jnp.where(take, other, mine) >> 1) + depth_shift
                out_c[h] = color.astype(out_c.dtype)
            for band in range(bands):
                summed = jnp.sum(color[:, 8 * band : 8 * band + 8], axis=1)
                spread = (place == lane + (h * bands + band) * blocks).astype(jnp.float32)
                total = total + jnp.dot(
                    summed,
                    spread,
                    precision=lax.Precision.HIGHEST,
                    preferred_element_type=jnp.float32,
                )
        for channel in range(3):
            thumb_ref[channel, region : region + 1] = total[channel : channel + 1] * (1.0 / 64.0)


def order_kernel(rank_ref, owner_ref, table_ref, thumb_ref, out_ref):
    rank = rank_ref[0]

    def body(r, carry):
        place = table_ref[owner_ref[r] ^ rank]
        for channel in range(3):
            out_ref[channel, pl.ds(r, 1)] = thumb_ref[channel, pl.ds(place, 1)]
        return carry

    lax.fori_loop(0, out_ref.shape[1], body, 0, unroll=4)


def shards(slot_tiles, owner_map, slot_depth, slot_color):
    grid_rows = lax.axis_size("gx")
    grid_cols = lax.axis_size("gy")
    ranks = grid_rows * grid_cols
    slots, rows, lanes = slot_depth.shape[1:]
    masks = exchange_plan(grid_rows, grid_cols)
    rank = (lax.axis_index("gx") * grid_cols + lax.axis_index("gy")).astype(jnp.int32)[None]
    depth = slot_depth[0]
    color = jnp.transpose(slot_color[0], (0, 2, 1, 3))

    def d_shape(n):
        return jax.ShapeDtypeStruct((n, rows, lanes), jnp.int32)

    def c_shape(n):
        return jax.ShapeDtypeStruct((n, 3, rows, lanes), color.dtype)

    def swap(array, mask):
        return lax.ppermute(array, axes, [(p, p ^ mask) for p in range(ranks)])

    keep_d, keep_c, send_d, send_c = pl.pallas_call(
        lambda *refs: pack_kernel(grid_cols, *refs),
        out_shape=[d_shape(ranks), c_shape(ranks), d_shape(ranks), c_shape(ranks)],
        in_specs=[smem, smem, smem, smem, vmem, vmem],
        out_specs=[vmem] * 4,
        scratch_shapes=[pltpu.SMEM((2 * ranks,), jnp.int32)],
        name="pack",
    )(rank, slot_tiles, owner_map, jnp.asarray(position_table(masks, ranks)), depth, color)

    count = ranks
    for step, mask in enumerate(masks[:-1]):
        got_d, got_c = swap(send_d, mask), swap(send_c, mask)
        bit = mask.bit_length() - 1
        kind = "key" if step == 0 else ("order" if mask < grid_cols else "depth")
        final = step == len(masks) - 2
        half = count // 2
        shapes = [d_shape(count), c_shape(count)] if final else [d_shape(half), c_shape(half)] * 2
        merged = pl.pallas_call(
            lambda *refs, bit=bit, kind=kind: merge_kernel(bit, kind, *refs),
            out_shape=shapes,
            in_specs=[smem, vmem, vmem, vmem, vmem],
            out_specs=[vmem] * len(shapes),
            name="merge",
        )(rank, keep_d, keep_c, got_d, got_c)
        keep_d, keep_c = merged[:2]
        if not final:
            send_d, send_c = merged[2:]
            count = half

    mask = masks[-1]
    width = 2 * rows * lanes // 64
    merged_d, merged_c, thumbs = pl.pallas_call(
        lambda *refs: last_kernel(mask.bit_length() - 1, *refs),
        out_shape=[d_shape(2), c_shape(2), jax.ShapeDtypeStruct((3, 2, width), jnp.float32)],
        in_specs=[smem, vmem, vmem, vmem, vmem],
        out_specs=[vmem] * 3,
        name="last",
    )(rank, keep_d, keep_c, swap(keep_d, mask), swap(keep_c, mask))

    spread = [mask] + masks[1:-1] + masks[:1]
    for mask in spread[1:]:
        thumbs = jnp.concatenate([thumbs, swap(thumbs, mask)], axis=1)
    thumbnail = pl.pallas_call(
        order_kernel,
        out_shape=jax.ShapeDtypeStruct(thumbs.shape, jnp.float32),
        in_specs=[smem, smem, smem, vmem],
        out_specs=vmem,
        name="order",
    )(rank, owner_map, jnp.asarray(gather_table(spread, ranks)), thumbs)
    return (
        merged_d[None],
        jnp.transpose(merged_c, (0, 2, 1, 3))[None],
        jnp.transpose(thumbnail, (1, 0, 2)),
    )


def solution(mesh):
    placed = (
        P(axes, None),
        P(),
        P(axes, None, None, None),
        P(axes, None, None, None, None),
    )
    return jax.shard_map(
        shards,
        mesh=mesh,
        in_specs=placed,
        out_specs=(P(axes, None, None, None), P(axes, None, None, None, None), P()),
        check_vma=False,
    )
```

```python
import jax
import jax.numpy as jnp
import numpy as np
from jax import lax
from jax.experimental import pallas as pl
from jax.experimental.pallas import tpu as pltpu
from jax.sharding import PartitionSpec as P

far_depth = 1073741824
depth_shift = 536870912
last_key = 2147483647
axes = ("gx", "gy")
smem = pl.BlockSpec(memory_space=pltpu.SMEM)
vmem = pl.BlockSpec(memory_space=pltpu.VMEM)


def exchange_plan(grid_rows, grid_cols):
    col_masks = [1 << i for i in range(grid_cols.bit_length() - 1)]
    row_masks = [grid_cols << i for i in range(1, grid_rows.bit_length() - 1)]
    tag_bits = 2 if len(row_masks) == 1 else 1
    rest = row_masks + col_masks if tag_bits == 2 else col_masks + row_masks
    stages = [[grid_cols]]
    if tag_bits == 1 and len(col_masks) % 2:
        stages.append(rest[:1])
        rest = rest[1:]
    stages += [rest[i : i + 2] for i in range(0, len(rest), 2)]
    return stages, tag_bits


def partners(stage):
    if len(stage) == 1:
        return [0, stage[0]]
    return [0, stage[0], stage[1], stage[0] ^ stage[1]]


def place_table(masks, ranks):
    table = np.zeros((ranks,), np.int32)
    for place in range(ranks):
        x = 0
        for bit, mask in enumerate(masks):
            if place >> bit & 1:
                x ^= mask
        table[x] = place
    return table


def pack_kernel(grid_cols, tag_bits, rank_ref, tiles_ref, owner_ref, table_ref, depth_ref, color_ref, *refs):
    outs, source_ref = refs[:-1], refs[-1]
    slots = depth_ref.shape[0]
    half = outs[0].shape[0]

    def clear(p, carry):
        source_ref[p] = -1
        return carry

    lax.fori_loop(0, 2 * half, clear, 0, unroll=8)
    rank = rank_ref[0]
    tag = lax.div(rank, grid_cols) & ((1 << tag_bits) - 1)

    def place(i, carry):
        tile = tiles_ref[0, i]

        @pl.when(tile >= 0)
        def _():
            row = lax.div(tile, grid_cols)
            col = lax.rem(tile, grid_cols)
            owner = owner_ref[(row >> 1) * grid_cols + col]
            source_ref[table_ref[owner ^ rank] * 2 + (row & 1)] = i

        return carry

    lax.fori_loop(0, slots, place, 0, unroll=4)

    def move(base, out_d, out_c):
        def body(p, carry):
            source = source_ref[base + p]
            used = source >= 0
            slot = jnp.maximum(source, 0)
            key = ((depth_ref[slot] - depth_shift) << tag_bits) + tag
            out_d[p] = jnp.where(used, key, last_key)
            color = color_ref[slot]
            out_c[p] = jnp.where(used, color, jnp.full_like(color, -1))
            return carry

        lax.fori_loop(0, half, body, 0, unroll=4)

    move(half, outs[2], outs[3])
    move(0, outs[0], outs[1])


def nearer(first, second, later, shift):
    key_a, color_a = first
    key_b, color_b = second
    cmp_a, cmp_b = key_a >> shift, key_b >> shift
    on_tie = jnp.where(later == 1, color_b[0], -1.0 - color_a[0]) >= 0
    take = (cmp_b < cmp_a) | ((cmp_b == cmp_a) & on_tie)
    return jnp.where(take, key_b, key_a), jnp.where(take[None], color_b, color_a)


def merge_tiles(stage, shift, rank, refs, index_of):
    later = [(rank >> (mask.bit_length() - 1)) & 1 for mask in stage]
    items = []
    for k in range(len(refs) // 2):
        p = index_of(k)
        items.append((refs[2 * k][p], refs[2 * k + 1][p].astype(jnp.float32)))
    level = 0
    while len(items) > 1:
        items = [nearer(items[i], items[i + 1], later[level], shift) for i in range(0, len(items), 2)]
        level += 1
    return items[0]


def merge_kernel(stage, shift, rank_ref, *refs):
    sources = 2 * len(partners(stage))
    ins, outs = refs[:sources], refs[sources:]
    rank = rank_ref[0]
    size = outs[0].shape[0]
    for part in reversed(range(len(outs) // 2)):

        def body(p, carry, part=part):
            key, color = merge_tiles(stage, shift, rank, ins, lambda k: part * size + p)
            outs[2 * part][p] = key
            outs[2 * part + 1][p] = color.astype(outs[1].dtype)
            return carry

        lax.fori_loop(0, size, body, 0, unroll=2)


def last_kernel(stage, shift, tag_bits, rank_ref, *refs):
    ins, (out_d, out_c, thumb_ref) = refs[:-3], refs[-3:]
    rank = rank_ref[0]
    rows, lanes = out_d.shape[-2:]
    blocks = lanes // 8
    bands = rows // 8
    width = 2 * bands * blocks
    lane = lax.broadcasted_iota(jnp.int32, (lanes, width), 0) // 8
    place = lax.broadcasted_iota(jnp.int32, (lanes, width), 1)
    total = jnp.zeros((3, width), jnp.float32)
    for h in range(2):
        key, color = merge_tiles(stage, shift, rank, ins, lambda k: h)
        empty = color[0] < 0
        out_d[h] = jnp.where(empty, far_depth, (key >> tag_bits) + depth_shift)
        color = jnp.where(empty[None], 0.0, color)
        out_c[h] = color.astype(out_c.dtype)
        for band in range(bands):
            summed = jnp.sum(color[:, 8 * band : 8 * band + 8], axis=1)
            spread = (place == lane + (h * bands + band) * blocks).astype(jnp.float32)
            total = total + jnp.dot(
                summed,
                spread,
                precision=lax.Precision.HIGHEST,
                preferred_element_type=jnp.float32,
            )
    for channel in range(3):
        thumb_ref[channel] = total[channel : channel + 1] * (1.0 / 64.0)


def order_kernel(rank_ref, owner_ref, table_ref, own_ref, got_ref, out_ref):
    rank = rank_ref[0]
    half = own_ref.shape[1]

    def body(r, carry):
        place = table_ref[owner_ref[r] ^ rank]
        mine = place < half
        row = jnp.where(mine, place, place - half)
        for channel in range(3):
            out_ref[channel, pl.ds(r, 1)] = jnp.where(
                mine, own_ref[channel, pl.ds(row, 1)], got_ref[channel, pl.ds(row, 1)]
            )
        return carry

    lax.fori_loop(0, out_ref.shape[1], body, 0, unroll=4)


def shards(slot_tiles, owner_map, slot_depth, slot_color):
    grid_rows = lax.axis_size("gx")
    grid_cols = lax.axis_size("gy")
    ranks = grid_rows * grid_cols
    rows, lanes = slot_depth.shape[2:]
    stages, tag_bits = exchange_plan(grid_rows, grid_cols)
    rank = (lax.axis_index("gx") * grid_cols + lax.axis_index("gy")).astype(jnp.int32)[None]
    depth = slot_depth[0]
    color = jnp.transpose(slot_color[0], (0, 2, 1, 3))

    def pair_shape(n):
        return [
            jax.ShapeDtypeStruct((n, rows, lanes), jnp.int32),
            jax.ShapeDtypeStruct((n, 3, rows, lanes), color.dtype),
        ]

    def swap(array, mask):
        return lax.ppermute(array, axes, [(p, p ^ mask) for p in range(ranks)])

    order = [mask for stage in reversed(stages) for mask in stage]
    parts = pl.pallas_call(
        lambda *refs: pack_kernel(grid_cols, tag_bits, *refs),
        out_shape=pair_shape(ranks) * 2,
        in_specs=[smem, smem, smem, smem, vmem, vmem],
        out_specs=[vmem] * 4,
        scratch_shapes=[pltpu.SMEM((2 * ranks,), jnp.int32)],
        name="pack",
    )(rank, slot_tiles, owner_map, jnp.asarray(place_table(order, ranks)), depth, color)

    count = ranks
    for step, stage in enumerate(stages):
        shift = 1 if tag_bits == 1 and stage[-1] > grid_cols else 0
        masks = partners(stage)
        operands = list(parts[:2])
        for k in range(1, len(masks)):
            operands += [swap(parts[2 * k], masks[k]), swap(parts[2 * k + 1], masks[k])]
        specs = dict(in_specs=[smem] + [vmem] * len(operands))
        if step + 1 < len(stages):
            split = 1 << len(stages[step + 1])
            count //= split
            shapes = pair_shape(count) * split
            parts = pl.pallas_call(
                lambda *refs, stage=stage, shift=shift: merge_kernel(stage, shift, *refs),
                out_shape=shapes,
                out_specs=[vmem] * len(shapes),
                name="merge",
                **specs,
            )(rank, *operands)
        else:
            width = 2 * rows * lanes // 64
            merged_d, merged_c, thumbs = pl.pallas_call(
                lambda *refs: last_kernel(stage, shift, tag_bits, *refs),
                out_shape=pair_shape(2) + [jax.ShapeDtypeStruct((3, 1, width), jnp.float32)],
                out_specs=[vmem] * 3,
                name="last",
                **specs,
            )(rank, *operands)

    for stage in reversed(stages[1:]):
        thumbs = jnp.concatenate([thumbs] + [swap(thumbs, m) for m in partners(stage)[1:]], axis=1)
    got = swap(thumbs, stages[0][0])
    thumbnail = pl.pallas_call(
        order_kernel,
        out_shape=jax.ShapeDtypeStruct((3, ranks, thumbs.shape[2]), jnp.float32),
        in_specs=[smem, smem, smem, vmem, vmem],
        out_specs=vmem,
        name="order",
    )(rank, owner_map, jnp.asarray(place_table(order, ranks)), thumbs, got)
    return (
        merged_d[None],
        jnp.transpose(merged_c, (0, 2, 1, 3))[None],
        jnp.transpose(thumbnail, (1, 0, 2)),
    )


def solution(mesh):
    placed = (
        P(axes, None),
        P(),
        P(axes, None, None, None),
        P(axes, None, None, None, None),
    )
    return jax.shard_map(
        shards,
        mesh=mesh,
        in_specs=placed,
        out_specs=(P(axes, None, None, None), P(axes, None, None, None, None), P()),
        check_vma=False,
    )
```

```python
import jax
import jax.numpy as jnp
import numpy as np
from jax import lax
from jax.experimental import pallas as pl
from jax.experimental.pallas import tpu as pltpu
from jax.sharding import PartitionSpec as P


far_depth = 1073741824
depth_shift = 536870912
last_key = 2147483647
axes = ("gx", "gy")
smem = pl.BlockSpec(memory_space=pltpu.SMEM)
vmem = pl.BlockSpec(memory_space=pltpu.VMEM)


def exchange_plan(grid_rows, grid_cols):
    col_masks = [1 << i for i in range(grid_cols.bit_length() - 1)]
    row_masks = [grid_cols << i for i in range(1, grid_rows.bit_length() - 1)]
    tag_bits = 2 if len(row_masks) == 1 else 1
    rest = row_masks + col_masks if tag_bits == 2 else col_masks + row_masks
    stages = [[grid_cols]]
    if tag_bits == 1 and len(col_masks) % 2:
        stages.append(rest[:1])
        rest = rest[1:]
    stages += [rest[i : i + 2] for i in range(0, len(rest), 2)]
    return stages, tag_bits


def partners(stage):
    if len(stage) == 1:
        return [0, stage[0]]
    return [0, stage[0], stage[1], stage[0] ^ stage[1]]


def place_table(masks, ranks):
    table = np.zeros((ranks,), np.int32)
    for place in range(ranks):
        x = 0
        for bit, mask in enumerate(masks):
            if place >> bit & 1:
                x ^= mask
        table[x] = place
    return table


def pack_kernel(grid_cols, tag_bits, base, rank_ref, tiles_ref, owner_ref, table_ref, depth_ref, color_ref, *refs):
    out_d, out_c, source_ref = refs
    slots = depth_ref.shape[0]
    half = out_d.shape[0]

    def clear(p, carry):
        source_ref[p] = -1
        return carry

    lax.fori_loop(0, 2 * half, clear, 0, unroll=8)
    rank = rank_ref[0]
    tag = lax.div(rank, grid_cols) & ((1 << tag_bits) - 1)

    def place(i, carry):
        tile = tiles_ref[0, i]

        @pl.when(tile >= 0)
        def _():
            row = lax.div(tile, grid_cols)
            col = lax.rem(tile, grid_cols)
            owner = owner_ref[(row >> 1) * grid_cols + col]
            source_ref[table_ref[owner ^ rank] * 2 + (row & 1)] = i

        return carry

    lax.fori_loop(0, slots, place, 0, unroll=4)

    def move(p, carry):
        source = source_ref[base + p]
        used = source >= 0
        slot = jnp.maximum(source, 0)
        key = ((depth_ref[slot] - depth_shift) << tag_bits) + tag
        out_d[p] = jnp.where(used, key, last_key)
        color = color_ref[slot]
        out_c[p] = jnp.where(used, color, jnp.full_like(color, -1))
        return carry

    lax.fori_loop(0, half, move, 0, unroll=4)


def nearer(first, second, later, shift):
    key_a, color_a = first
    key_b, color_b = second
    cmp_a, cmp_b = key_a >> shift, key_b >> shift
    on_tie = jnp.where(later == 1, color_b[0], -1.0 - color_a[0]) >= 0
    take = (cmp_b < cmp_a) | ((cmp_b == cmp_a) & on_tie)
    return jnp.where(take, key_b, key_a), jnp.where(take[None], color_b, color_a)


def merge_tiles(stage, shift, rank, refs, index_of):
    later = [(rank >> (mask.bit_length() - 1)) & 1 for mask in stage]
    items = []
    for k in range(len(refs) // 2):
        p = index_of(k)
        items.append((refs[2 * k][p], refs[2 * k + 1][p].astype(jnp.float32)))
    level = 0
    while len(items) > 1:
        items = [nearer(items[i], items[i + 1], later[level], shift) for i in range(0, len(items), 2)]
        level += 1
    return items[0]


def merge_kernel(stage, shift, first, rank_ref, *refs):
    sources = 2 * len(partners(stage))
    ins, outs = refs[:sources], refs[sources:]
    rank = rank_ref[0]
    size = outs[0].shape[0]
    for place in range(len(outs) // 2):

        def body(p, carry, place=place):
            key, color = merge_tiles(stage, shift, rank, ins, lambda k: (first + place) * size + p)
            outs[2 * place][p] = key
            outs[2 * place + 1][p] = color.astype(outs[1].dtype)
            return carry

        lax.fori_loop(0, size, body, 0, unroll=2)


def last_kernel(stage, shift, tag_bits, rank_ref, *refs):
    ins, (out_d, out_c, thumb_ref) = refs[:-3], refs[-3:]
    rank = rank_ref[0]
    rows, lanes = out_d.shape[-2:]
    blocks = lanes // 8
    bands = rows // 8
    width = 2 * bands * blocks
    lane = lax.broadcasted_iota(jnp.int32, (lanes, width), 0) // 8
    place = lax.broadcasted_iota(jnp.int32, (lanes, width), 1)
    total = jnp.zeros((3, width), jnp.float32)
    for h in range(2):
        key, color = merge_tiles(stage, shift, rank, ins, lambda k: h)
        empty = color[0] < 0
        out_d[h] = jnp.where(empty, far_depth, (key >> tag_bits) + depth_shift)
        color = jnp.where(empty[None], 0.0, color)
        out_c[h] = color.astype(out_c.dtype)
        for band in range(bands):
            summed = jnp.sum(color[:, 8 * band : 8 * band + 8], axis=1)
            spread = (place == lane + (h * bands + band) * blocks).astype(jnp.float32)
            total = total + jnp.dot(
                summed,
                spread,
                precision=lax.Precision.HIGHEST,
                preferred_element_type=jnp.float32,
            )
    for channel in range(3):
        thumb_ref[channel] = total[channel : channel + 1] * (1.0 / 64.0)


def order_kernel(rank_ref, owner_ref, table_ref, own_ref, got_ref, out_ref):
    rank = rank_ref[0]
    half = own_ref.shape[1]

    def body(r, carry):
        place = table_ref[owner_ref[r] ^ rank]
        mine = place < half
        row = jnp.where(mine, place, place - half)
        for channel in range(3):
            out_ref[channel, pl.ds(r, 1)] = jnp.where(
                mine, own_ref[channel, pl.ds(row, 1)], got_ref[channel, pl.ds(row, 1)]
            )
        return carry

    lax.fori_loop(0, out_ref.shape[1], body, 0, unroll=4)


def composite(slot_tiles, owner_map, slot_depth, slot_color):
    grid_rows = lax.axis_size("gx")
    grid_cols = lax.axis_size("gy")
    ranks = grid_rows * grid_cols
    rows, lanes = slot_depth.shape[2:]
    stages, tag_bits = exchange_plan(grid_rows, grid_cols)
    rank = (lax.axis_index("gx") * grid_cols + lax.axis_index("gy")).astype(jnp.int32)[None]
    depth = slot_depth[0]
    color = jnp.transpose(slot_color[0], (0, 2, 1, 3))

    def pair_shape(n):
        return [
            jax.ShapeDtypeStruct((n, rows, lanes), jnp.int32),
            jax.ShapeDtypeStruct((n, 3, rows, lanes), color.dtype),
        ]

    def swap(array, mask):
        return lax.ppermute(array, axes, [(p, p ^ mask) for p in range(ranks)])

    order = [mask for stage in reversed(stages) for mask in stage]
    table = jnp.asarray(place_table(order, ranks))

    def pack(base):
        return pl.pallas_call(
            lambda *refs: pack_kernel(grid_cols, tag_bits, base, *refs),
            out_shape=pair_shape(ranks),
            in_specs=[smem, smem, smem, smem, vmem, vmem],
            out_specs=[vmem] * 2,
            scratch_shapes=[pltpu.SMEM((2 * ranks,), jnp.int32)],
            name="pack",
        )(rank, slot_tiles, owner_map, table, depth, color)

    sends = pack(ranks)
    parts = list(pack(0)) + list(sends)

    count = ranks
    for step, stage in enumerate(stages):
        shift = 1 if tag_bits == 1 and stage[-1] > grid_cols else 0
        masks = partners(stage)
        operands = list(parts[:2])
        for k in range(1, len(masks)):
            operands += [swap(parts[2 * k], masks[k]), swap(parts[2 * k + 1], masks[k])]
        specs = dict(in_specs=[smem] + [vmem] * len(operands))
        if step + 1 < len(stages):
            split = 1 << len(stages[step + 1])
            count //= split

            def merge(first, number):
                return pl.pallas_call(
                    lambda *refs: merge_kernel(stage, shift, first, *refs),
                    out_shape=pair_shape(count) * number,
                    out_specs=[vmem] * (2 * number),
                    name="merge",
                    **specs,
                )(rank, *operands)

            sends = merge(1, split - 1)
            parts = list(merge(0, 1)) + list(sends)
        else:
            width = 2 * rows * lanes // 64
            merged_d, merged_c, thumbs = pl.pallas_call(
                lambda *refs: last_kernel(stage, shift, tag_bits, *refs),
                out_shape=pair_shape(2) + [jax.ShapeDtypeStruct((3, 1, width), jnp.float32)],
                out_specs=[vmem] * 3,
                name="last",
                **specs,
            )(rank, *operands)

    for stage in reversed(stages[1:]):
        thumbs = jnp.concatenate([thumbs] + [swap(thumbs, m) for m in partners(stage)[1:]], axis=1)
    got = swap(thumbs, stages[0][0])
    thumbnail = pl.pallas_call(
        order_kernel,
        out_shape=jax.ShapeDtypeStruct((3, ranks, thumbs.shape[2]), jnp.float32),
        in_specs=[smem, smem, smem, vmem, vmem],
        out_specs=vmem,
        name="order",
    )(rank, owner_map, table, thumbs, got)
    return (
        merged_d[None],
        jnp.transpose(merged_c, (0, 2, 1, 3))[None],
        jnp.transpose(thumbnail, (1, 0, 2)),
    )


def solution(mesh):
    placed = (
        P(axes, None),
        P(),
        P(axes, None, None, None),
        P(axes, None, None, None, None),
    )
    return jax.shard_map(
        composite,
        mesh=mesh,
        in_specs=placed,
        out_specs=(P(axes, None, None, None), P(axes, None, None, None, None), P()),
        check_vma=False,
    )
```
